256 devices in a mesh: seq: 32 (over y, z), head: 8 (over x, core).
Axes of the slice: x: 4, y: 4, z: 8, core: 2. Of those that a mesh axis runs over, the one named last changes fastest.
Arguments:
- tokens: bfloat16 [32768, 2048], P(('seq', 'head')), may hold values from -6 to 6
- w_in_x: bfloat16 [2048, 4096], P(None, 'head'), may hold values from -0.125 to 0.125
- w_in_z: bfloat16 [2048, 4096], P(None, 'head'), may hold values from -0.125 to 0.125
- w_in_bc: bfloat16 [2048, 256], replicated, may hold values from -0.125 to 0.125
- w_dt: bfloat16 [2048, 64], P(None, 'head'), may hold values from -0.125 to 0.125
- conv_x: float32 [4, 4096], P(None, 'head'), may hold values from -3 to 3
- conv_bc: float32 [4, 256], replicated, may hold values from -3 to 3
- dt_bias: float32 [64], P('head'), may hold values from -1 to 1
- decay_rate: float32 [64], P('head'), may hold values from 1.5258789e-06 to 0.05, as said below
- skip: float32 [64], P('head'), may hold values from 0.5 to 1.5
- norm_gain: float32 [4096], P('head'), may hold values from 0.25 to 1.75
- w_out: bfloat16 [4096, 2048], P('head'), may hold values from -0.09375 to 0.09375
Outputs:
- mixed: bfloat16 [32768, 2048], P(('seq', 'head'))
The draws below stay inside these ranges and needn't reach their ends.
Inputs may be any that keep to these rules, and one draw needn't show every extreme that they name: `decay_rate`: positive per-head decay rates.
All inputs are finite; a program needn't handle non-finite values.
Results may differ from the reference program's by a relative error of at most 0.013.
Values may be sent and summed in bfloat16 or wider, within the bound.
No kernel may reach another device: no remote copies, remote signals or barrier semaphores. Data moves between devices by JAX's collectives and lax.ppermute only.
A program may use at most 128 MiB of HBM per device.

```python
import math
import jax
import jax.numpy as jnp
from jax import lax

D = 2048
H = 64
HEADDIM = 64
STATE = 128
SPAN = 256
KERNEL = 4
E = 4096
TOKENS = 32768
N_HEAD = 8


def draw_decay_rate(key, part):
    lowest = 0.05 / TOKENS
    return jnp.exp(jax.random.uniform(jax.random.fold_in(key, 14), (H,), minval=math.log(lowest), maxval=math.log(0.05))).astype(jnp.float32)


def shard_levels(own_key, extent, cuts, least, largest):
    gain = 1.0
    for dim, blocks in cuts:
        steps = jax.random.uniform(jax.random.fold_in(jax.random.fold_in(own_key, 6), dim), (blocks,), jnp.float32, least / len(cuts), largest / len(cuts))
        gain = gain * jnp.repeat(jnp.exp(steps), extent[dim] // blocks).reshape((-1,) + (1,) * (len(extent) - 1 - dim))
    return gain


def bell_draw(own_key, dims, scale, limit, cuts=(), kind=jnp.bfloat16):
    entries = jax.random.normal(own_key, dims, jnp.float32) * scale
    if len(cuts) > 0:
        entries = shard_levels(own_key, dims, cuts, -0.22, 0.18) * entries
    return jnp.clip(entries, min=-limit, max=limit).astype(kind)


def setup_inputs(seed: int = 0) -> dict:
    key_list = jax.random.split(jax.random.key(seed), 13)
    return {
        "tokens": bell_draw(key_list[0], (TOKENS, D), 1.0, 6.0, ((0, 256),)),
        "w_in_x": bell_draw(key_list[1], (D, E), D ** -0.5, 0.125, ((1, 8),)),
        "w_in_z": bell_draw(key_list[2], (D, E), D ** -0.5, 0.125, ((1, 8),)),
        "w_in_bc": bell_draw(key_list[3], (D, 2 * STATE), D ** -0.5, 0.125),
        "w_dt": bell_draw(key_list[4], (D, H), D ** -0.5, 0.125, ((1, 8),)),
        "conv_x": bell_draw(key_list[5], (KERNEL, E), KERNEL ** -0.5, 3.0, ((1, 8),), jnp.float32),
        "conv_bc": bell_draw(key_list[6], (KERNEL, 2 * STATE), KERNEL ** -0.5, 3.0, (), jnp.float32),
        "dt_bias": jnp.clip(jax.random.uniform(key_list[7], (H,), jnp.float32, -1.0, 1.0) * shard_levels(key_list[7], (H,), ((0, 8),), -0.4, 0.0), -1.0, 1.0),
        "decay_rate": draw_decay_rate(jax.random.fold_in(key_list[12], 71), 0),
        "skip": jnp.clip(0.5 + 1.0 * jax.random.uniform(key_list[9], (H,), jnp.float32) ** shard_levels(key_list[9], (H,), ((0, 8),), -0.2, 0.2), 0.5, 1.5),
        "norm_gain": jnp.clip(1.0 + 0.15 * jax.random.normal(key_list[10], (E,), jnp.float32), 0.25, 1.75),
        "w_out": bell_draw(key_list[11], (E, D), E ** -0.5, 0.09375, ((0, 8),)),
    }


highest = lax.Precision.HIGHEST

def span_update(state, x_span, step_span, decay_span, b_span, c_span, skip):
    cumul = jnp.cumsum(decay_span, axis=0)
    length = x_span.shape[0]
    lower = jnp.arange(length)[:, None] >= jnp.arange(length)[None, :]
    spread = cumul.T[:, :, None] - cumul.T[:, None, :]
    within = jnp.exp(jnp.where(lower[None], spread, -jnp.inf))
    scores = jnp.dot(c_span, b_span.T, precision=highest)
    scaled = x_span * step_span[:, :, None]
    output = jnp.einsum('hts,shp->thp', within * scores[None], scaled, precision=highest)
    output = output + jnp.einsum('tn,hpn->thp', c_span, state, precision=highest) * jnp.exp(cumul)[:, :, None]
    output = output + skip[None, :, None] * x_span
    remain = jnp.exp(cumul[-1][None, :] - cumul)
    fresh = jnp.einsum('shp,sn->hpn', scaled * remain[:, :, None], b_span, precision=highest)
    return (jnp.exp(cumul[-1])[:, None, None] * state + fresh, output, cumul)

def causal_conv(values, before, kernel):
    padded = jnp.concatenate([before, values], axis=0)
    length = values.shape[0]
    result = kernel[0] * padded[0:length]
    for offset in range(1, kernel.shape[0]):
        result = result + kernel[offset] * padded[offset:offset + length]
    return jax.nn.silu(result)

def reference(tokens, w_in_x, w_in_z, w_in_bc, w_dt, conv_x, conv_bc, dt_bias, decay_rate, skip, norm_gain, w_out):
    x_proj = jnp.dot(tokens, w_in_x, preferred_element_type=jnp.float32)
    gate_proj = jnp.dot(tokens, w_in_z, preferred_element_type=jnp.float32)
    bc_proj = jnp.dot(tokens, w_in_bc, preferred_element_type=jnp.float32)
    step_raw = jnp.dot(tokens, w_dt, preferred_element_type=jnp.float32)
    x_conv = causal_conv(x_proj, jnp.zeros((KERNEL - 1, x_proj.shape[1]), jnp.float32), conv_x)
    bc_conv = causal_conv(bc_proj, jnp.zeros((KERNEL - 1, bc_proj.shape[1]), jnp.float32), conv_bc)
    step_size = jax.nn.softplus(step_raw + dt_bias)
    log_decay = -step_size * decay_rate
    spans = TOKENS // SPAN

    def advance(state, inputs):
        x_span, step_span, decay_span, bc_span = inputs
        state, output, cumul = span_update(state, x_span, step_span, decay_span, bc_span[:, :STATE], bc_span[:, STATE:], skip)
        return (state, output)
    initial = jnp.zeros((H, HEADDIM, STATE), jnp.float32)
    final_state, outputs = lax.scan(advance, initial, (x_conv.reshape(spans, SPAN, H, HEADDIM), step_size.reshape(spans, SPAN, H), log_decay.reshape(spans, SPAN, H), bc_conv.reshape(spans, SPAN, 2 * STATE)))
    ssd_out = outputs.reshape(TOKENS, E)
    gated = ssd_out * jax.nn.silu(gate_proj)
    meansq = lax.optimization_barrier(jnp.mean(gated * gated, axis=1))
    normed = (gated * lax.rsqrt(meansq + 1e-05)[:, None] * norm_gain).astype(jnp.bfloat16)
    share = E // N_HEAD
    summed = jnp.zeros((TOKENS, D), jnp.float32)
    for member in range(N_HEAD):
        partial_term = jnp.dot(normed[:, member * share:(member + 1) * share], w_out[member * share:(member + 1) * share], preferred_element_type=jnp.float32).astype(jnp.bfloat16)
        summed = summed + lax.optimization_barrier(partial_term).astype(jnp.float32)
    return summed.astype(jnp.bfloat16)
```

```python
import jax
import jax.numpy as jnp
from jax import lax
from jax.experimental import pallas as pl
from jax.experimental.pallas import tpu as pltpu
from jax.sharding import Mesh
from jax.sharding import PartitionSpec as P


E = 4096
Q = 128
KERNEL = 4
SEQ = ("y", "z")
ALL = ("y", "z", "x", "c")
F32 = jnp.float32
BF16 = jnp.bfloat16
highest = lax.Precision.HIGHEST


def silu(v):
    half = 0.5 * v
    return half + half * jnp.tanh(half)


def shift(block, axis, distance):
    size = lax.axis_size(axis)
    return lax.ppermute(block, axis, [(i, (i + distance) % size) for i in range(size)])


def later(block, axis, distance):
    size = lax.axis_size(axis)
    return lax.ppermute(block, axis, [(i, i + distance) for i in range(size - distance)])


def fold(values, heads, chunk):
    lanes = values.shape[1]
    high = values.astype(BF16).astype(F32)
    low = values - high
    first = pltpu.roll(high, -chunk * heads % lanes, 1) if chunk else high
    second = pltpu.roll(low, (heads - chunk * heads) % lanes, 1) if chunk != 1 else low
    lane = lax.broadcasted_iota(jnp.int32, values.shape, 1)
    return jnp.where(lane < heads, first, second).astype(BF16)


def widen(values, heads, chunk, spread):
    return jnp.dot(fold(values, heads, chunk), spread, preferred_element_type=F32)


def spread_of(heads, width):
    line = lax.broadcasted_iota(jnp.int32, (Q, width), 0)
    lane = lax.broadcasted_iota(jnp.int32, (Q, width), 1)
    hit = (line % heads == lane // (width // heads)) & (line < 2 * heads)
    return jnp.where(hit, 1.0, 0.0).astype(BF16)


def lanes_of(scalars, heads, limit):
    lane = lax.broadcasted_iota(jnp.int32, (1, Q), 1)
    row = jnp.zeros((1, Q), F32)
    for head in range(heads):
        row = jnp.where(lane % heads == head, scalars[head], row)
    return jnp.where(lane < limit, row, 0.0)


def starts_of(chunks):
    size = chunks // 2
    x_at, c_at = lax.axis_index("x"), lax.axis_index("c")
    places = []
    for distance in (0, size - 1, 1, 2):
        moved = x_at + distance
        place = jnp.where(moved >= size, moved - size, moved) * 2
        places += [(place + c_at) * Q, (place + 1 - c_at) * Q]
    return places


def three_rows(whole):
    row = lax.broadcasted_iota(jnp.int32, whole.shape, 0) % 16
    high = whole.astype(BF16).astype(F32)
    middle = (whole - high).astype(BF16).astype(F32)
    low = whole - high - middle
    return jnp.where(
        row == 0, high, jnp.where(row == 1, middle, jnp.where(row == 2, low, 0.0))
    ).astype(BF16)


def summary_kernel(heads, chunks):
    def kernel(
        bias, rate, g0, g1, g2, g3, halo, taps_x, taps_bc,
        xc_out, bc_out, dt_out, cum_out, last_out, window, scaled,
    ):
        width = xc_out.shape[1]
        conv_cols = width + bc_out.shape[1]
        starts = starts_of(chunks)
        for group, ref in enumerate((g0, g1, g2, g3)):
            for member in range(2):
                at = pl.multiple_of(starts[2 * group + member] + 8, 8)
                window[pl.ds(at, Q), :] = ref[member * Q : member * Q + Q, :]
        window[0:8, :conv_cols] = halo[...]
        spread = spread_of(heads, width)
        row = lax.broadcasted_iota(jnp.int32, (Q, Q), 0)
        col = lax.broadcasted_iota(jnp.int32, (Q, Q), 1)
        tri = jnp.where(row >= col, 1.0, 0.0)
        taps = jnp.concatenate([taps_x[...], taps_bc[...]], axis=1)
        lane = lax.broadcasted_iota(jnp.int32, (Q, Q), 1)
        raw = jnp.zeros((Q, Q), F32)
        for chunk in range(chunks):
            lo = 8 + chunk * Q
            part = window[lo : lo + Q, conv_cols:]
            part = pltpu.roll(part, chunk * heads, 1) if chunk else part
            raw = jnp.where(lane // heads == chunk, part, raw)
        raw = raw + lanes_of(bias, heads, chunks * heads)
        dt = jnp.maximum(raw, 0.0) + jnp.log1p(jnp.exp(-jnp.abs(raw)))
        log_decay = -dt * lanes_of(rate, heads, chunks * heads)
        cumul = jnp.dot(tri, log_decay, precision=highest, preferred_element_type=F32)
        dt_out[...] = dt
        cum_out[...] = cumul
        total = cumul[Q - 1 : Q, :]
        suffix = jnp.zeros((8, Q), F32)
        wide_total = jnp.broadcast_to(total, (8, Q))
        for k in range(1, chunks):
            suffix = suffix + pltpu.roll(wide_total, Q - k * heads, 1)
        suffix = suffix[0:1, :]
        weight = dt * jnp.exp(jnp.minimum(total - cumul + suffix, 0.0))
        for chunk in range(chunks):
            lo = 8 + chunk * Q
            conv = taps[3:4, :] * window[lo : lo + Q, :conv_cols]
            for back in range(1, KERNEL):
                conv += taps[3 - back : 4 - back, :] * window[lo - back : lo - back + Q, :conv_cols]
            act = silu(conv)
            xc_out[lo - 8 : lo - 8 + Q, :] = act[:, :width].astype(BF16)
            bc_out[lo - 8 : lo - 8 + Q, :] = act[:, width:].astype(BF16)
            wide = widen(weight, heads, chunk, spread)
            scaled[lo - 8 : lo - 8 + Q, :] = (act[:, :width] * wide).astype(BF16)
        last_out[:, :width] = lax.dot_general(
            bc_out[:, :Q], scaled[...], (((0,), (0,)), ((), ())), preferred_element_type=F32
        ).astype(BF16)
        last_out[:, width:] = three_rows(jnp.broadcast_to(total + suffix, (Q, Q)))

    return kernel


def vmem_specs(count, scalars=1):
    return [pl.BlockSpec(memory_space=pltpu.SMEM)] * scalars + [
        pl.BlockSpec(memory_space=pltpu.VMEM)
    ] * count


def summarize(bias, rate, groups, halo, taps_x, taps_bc, heads, width, bc_cols):
    rows = 8 * Q
    return pl.pallas_call(
        summary_kernel(heads, rows // Q),
        in_specs=vmem_specs(7, 2),
        out_shape=[
            jax.ShapeDtypeStruct((rows, width), BF16),
            jax.ShapeDtypeStruct((rows, bc_cols), BF16),
            jax.ShapeDtypeStruct((Q, Q), F32),
            jax.ShapeDtypeStruct((Q, Q), F32),
            jax.ShapeDtypeStruct((Q, width + Q), BF16),
        ],
        scratch_shapes=[
            pltpu.VMEM((rows + 8, groups[0].shape[1]), F32),
            pltpu.VMEM((rows, width), BF16),
        ],
        cost_estimate=pl.CostEstimate(
            flops=3_000_000_000, bytes_accessed=8_000_000, transcendentals=1_000_000
        ),
        name="summarize",
    )(bias, rate, *groups, halo, taps_x, taps_bc)


def inside_kernel(heads, chunks):
    def kernel(
        skip, g0, g1, g2, g3, xc, bc, dt_in, cum_in,
        ig_out, fz_out, sloc_out, growth_out, gate, flipped, decays, state,
    ):
        width = xc.shape[1]
        pair = 2 * (width // heads)
        spread = spread_of(heads, width)
        starts = starts_of(chunks)
        for group, ref in enumerate((g0, g1, g2, g3)):
            for member in range(2):
                at = pl.multiple_of(starts[2 * group + member], Q)
                gate[pl.ds(at, Q), :] = ref[member * Q : member * Q + Q, :]
        row = lax.broadcasted_iota(jnp.int32, (Q, Q), 0)
        col = lax.broadcasted_iota(jnp.int32, (Q, Q), 1)
        lower = row >= col
        lane = lax.broadcasted_iota(jnp.int32, (Q, pair), 1)
        zero = jnp.zeros((Q, pair), BF16)
        cumul = cum_in[...]
        flipped[...] = cumul.T
        total = cumul[Q - 1 : Q, :]
        wide_total = jnp.broadcast_to(total, (8, Q))
        prefix = jnp.zeros((8, Q), F32)
        for k in range(1, chunks):
            prefix = prefix + pltpu.roll(wide_total, k * heads, 1)
        grown = jnp.exp(prefix)
        decay = jnp.exp(wide_total)
        rows8 = lax.broadcasted_iota(jnp.int32, (8, Q), 0)
        grown_rows = jnp.zeros((8, Q), F32)
        decay_rows = jnp.zeros((8, Q), F32)
        for chunk in range(chunks):
            turn = -chunk * heads % Q
            grown_rows = jnp.where(
                rows8 == chunk, pltpu.roll(grown, turn, 1) if turn else grown, grown_rows
            )
            decay_rows = jnp.where(
                rows8 == chunk, pltpu.roll(decay, turn, 1) if turn else decay, decay_rows
            )
        growth_out[...] = widen(grown_rows, heads, 0, spread)
        decays[...] = widen(decay_rows, heads, 0, spread)
        state[...] = jnp.zeros((Q, width), F32)

        @pl.loop(0, chunks)
        def _(chunk):
            at = pl.ds(pl.multiple_of(chunk * Q, Q), Q)
            turn = lax.rem(Q - chunk * heads, Q)
            dt = pltpu.roll(dt_in[...], turn, 1)
            cumul = pltpu.roll(cum_in[...], turn, 1)
            rows = flipped[pl.ds(pl.multiple_of(chunk * heads, heads), heads), :]
            b_rows = bc[at, :Q]
            c_rows = bc[at, Q:]
            x = xc[at, :].astype(F32)
            sloc_out[chunk] = state[...].astype(BF16)
            weight = dt * jnp.exp(jnp.minimum(cumul[Q - 1 : Q, :] - cumul, 0.0))
            kept = (x * widen(weight, heads, 0, spread)).astype(BF16)
            fresh = lax.dot_general(
                b_rows, kept, (((0,), (0,)), ((), ())), preferred_element_type=F32
            )
            state[...] = decays[pl.ds(chunk, 1), :] * state[...] + fresh
            scores = lax.dot_general(
                c_rows, b_rows, (((1,), (1,)), ((), ())), preferred_element_type=F32
            )
            scores = jnp.where(lower, scores, 0.0)
            scaled = (x * widen(dt, heads, 0, spread)).astype(BF16)
            act = silu(gate[at, :])
            fz_out[at, :] = (widen(jnp.exp(cumul), heads, 0, spread) * act).astype(BF16)
            for first in range(0, heads, 2):
                parts = []
                for head in (first, first + 1):
                    gap = cumul[:, head : head + 1] - rows[head : head + 1, :]
                    parts.append((scores * jnp.exp(jnp.minimum(gap, 0.0))).astype(BF16))
                lo = (first // 2) * pair
                block = scaled[:, lo : lo + pair]
                stacked = jnp.concatenate(
                    [
                        jnp.where(lane < pair // 2, block, zero),
                        jnp.where(lane < pair // 2, zero, block),
                    ],
                    axis=0,
                )
                out = jnp.dot(
                    jnp.concatenate(parts, axis=1), stacked, preferred_element_type=F32
                )
                coefficient = jnp.where(lane < pair // 2, skip[first], skip[first + 1])
                out = out + coefficient * x[:, lo : lo + pair]
                ig_out[at, lo : lo + pair] = (out * act[:, lo : lo + pair]).astype(BF16)

    return kernel


def inside(skip, groups, xc, bc, dt, cumul, heads):
    rows, width = xc.shape
    chunks = rows // Q
    return pl.pallas_call(
        inside_kernel(heads, chunks),
        in_specs=vmem_specs(8),
        out_shape=[
            jax.ShapeDtypeStruct((rows, width), BF16),
            jax.ShapeDtypeStruct((rows, width), BF16),
            jax.ShapeDtypeStruct((chunks, Q, width), BF16),
            jax.ShapeDtypeStruct((8, width), F32),
        ],
        scratch_shapes=[
            pltpu.VMEM((rows, width), F32),
            pltpu.VMEM((Q, Q), F32),
            pltpu.VMEM((8, width), F32),
            pltpu.VMEM((Q, width), F32),
        ],
        cost_estimate=pl.CostEstimate(
            flops=8_000_000_000, bytes_accessed=8_000_000, transcendentals=2_000_000
        ),
        name="inside",
    )(skip, *groups, xc, bc, dt, cumul)


def finish_kernel(sel, c_rows, ig, fz, sloc, growth, entering, out):
    start = entering[...].astype(F32)
    first = 2 * pl.program_id(0)
    for i in range(2):
        chunk = 2 * (first + i) + sel[0]
        state = sloc[i, 0].astype(F32) + growth[pl.ds(chunk, 1), :] * start
        carried = jnp.dot(c_rows[i, 0], state.astype(BF16), preferred_element_type=F32)
        out[i * Q : i * Q + Q, :] = (
            ig[i, 0].astype(F32) + carried * fz[i, 0].astype(F32)
        ).astype(BF16)


def finish(sel, bc, ig, fz, sloc, growth, entering):
    rows, width = ig.shape
    pairs = rows // Q // 2
    paired = lambda block: block.reshape(pairs, 2, Q, -1)
    block = pl.BlockSpec((2, 1, Q, width), lambda i, sel: (i, sel[0], 0, 0))
    return pl.pallas_call(
        finish_kernel,
        grid_spec=pltpu.PrefetchScalarGridSpec(
            num_scalar_prefetch=1,
            grid=(pairs // 2,),
            in_specs=[
                pl.BlockSpec((2, 1, Q, Q), lambda i, sel: (i, sel[0], 0, 1)),
                block,
                block,
                block,
                pl.BlockSpec(growth.shape, lambda i, sel: (0, 0)),
                pl.BlockSpec(entering.shape, lambda i, sel: (0, 0)),
            ],
            out_specs=pl.BlockSpec((2 * Q, width), lambda i, sel: (i, 0)),
        ),
        out_shape=jax.ShapeDtypeStruct((rows // 2, width), BF16),
        cost_estimate=pl.CostEstimate(
            flops=1_500_000_000, bytes_accessed=3_000_000, transcendentals=0
        ),
        name="finish",
    )(sel, paired(bc), paired(ig), paired(fz), paired(sloc), growth, entering)


def row_kernel(heads):
    def kernel(pieces, before_out, growth_out, row_out):
        width = before_out.shape[2]
        spread = spread_of(heads, width)
        count = pieces.shape[0]
        rows8 = lax.broadcasted_iota(jnp.int32, (8, Q), 0)
        parts = jnp.zeros((8, Q), F32)
        sums = jnp.zeros((8, Q), F32)
        total = jnp.zeros((1, Q), F32)
        for k in range(count):
            tail = pieces[k, :, width:].astype(F32)
            part = tail[0:1] + tail[1:2] + tail[2:3]
            parts = jnp.where(rows8 == k, part, parts)
            sums = jnp.where(rows8 == k, total, sums)
            total = total + part
        growth_out[...] = widen(jnp.exp(sums), heads, 0, spread)
        decay = widen(jnp.exp(parts), heads, 0, spread)
        state = jnp.zeros(before_out.shape[1:], F32)
        for k in range(count):
            before_out[k] = state
            state = decay[k : k + 1] * state + pieces[k, :, :width].astype(F32)
        row_out[:, :width] = state.astype(BF16)
        row_out[:, width:] = three_rows(jnp.broadcast_to(total, (16, Q)))

    return kernel


def row_scan(pieces, heads):
    count, rows, cols = pieces.shape
    width = cols - Q
    return pl.pallas_call(
        row_kernel(heads),
        in_specs=vmem_specs(1, 0),
        out_shape=[
            jax.ShapeDtypeStruct((count, rows, width), F32),
            jax.ShapeDtypeStruct((8, width), F32),
            jax.ShapeDtypeStruct((rows, cols), BF16),
        ],
        name="row_scan",
    )(pieces)


def join_kernel(heads):
    def kernel(near, middle, far, before, growth, out):
        width = out.shape[2]
        spread = spread_of(heads, width)

        def log_of(piece):
            tail = piece[:, width:].astype(F32)
            return tail[0:1] + tail[1:2] + tail[2:3]

        rows8 = lax.broadcasted_iota(jnp.int32, (8, Q), 0)
        logs = jnp.where(rows8 == 0, log_of(near), log_of(middle))
        decay = widen(jnp.exp(logs), heads, 0, spread)
        entering = far[:, :width].astype(F32)
        entering = decay[1:2] * entering + middle[:, :width].astype(F32)
        entering = decay[0:1] * entering + near[:, :width].astype(F32)
        for k in range(out.shape[0]):
            out[k] = (before[k] + growth[k : k + 1] * entering).astype(BF16)

    return kernel


def join_rows(near, middle, far, before, growth, heads):
    count, rows, width = before.shape
    return pl.pallas_call(
        join_kernel(heads),
        in_specs=vmem_specs(5, 0),
        out_shape=jax.ShapeDtypeStruct((count, rows, width), BF16),
        name="join_rows",
    )(near, middle, far, before, growth)


def per_device(
    tokens, w_in_x, w_in_z, w_in_bc, w_dt, conv_x, conv_bc,
    dt_bias, decay_rate, skip, norm_gain, w_out,
):
    width = w_in_x.shape[1]
    heads = dt_bias.shape[0]
    bc_cols = w_in_bc.shape[1]
    own_rows, d_model = tokens.shape
    half = own_rows // 2
    x_size = lax.axis_size("x")
    x_at = lax.axis_index("x")
    c_at = lax.axis_index("c")
    swap = lambda block: shift(block, "c", 1)

    top, bottom = tokens[:half], tokens[half:]

    def named(block, distance, axis="x"):
        return shift(block, axis, distance)

    left_top = named(top, 1)
    right_bottom = named(bottom, -1)
    left_bottom = named(bottom, 1)
    right_top = named(top, -1)
    far_top = named(left_top, 1)
    far_bottom = named(right_bottom, -1)

    w_first = jnp.concatenate(
        [w_in_x, w_in_bc, w_dt, jnp.zeros((d_model, Q - heads), BF16)], axis=1
    )
    groups = (
        (0, (tokens, swap(tokens))),
        (
            -1,
            (
                left_top,
                left_bottom,
                named(left_top, 1, "c"),
                named(left_bottom, 1, "c"),
            ),
        ),
        (
            1,
            (
                right_top,
                right_bottom,
                named(right_top, 1, "c"),
                named(right_bottom, 1, "c"),
            ),
        ),
        (2, (far_top, far_bottom, swap(far_top), swap(far_bottom))),
    )
    conv_cols = width + bc_cols
    pairs, firsts = [], []
    edge = jnp.zeros((8, conv_cols), F32)
    for distance, blocks in groups:
        pair = jnp.concatenate(blocks, axis=0)
        first = jnp.dot(pair, w_first, preferred_element_type=F32)
        ends = [first[m * Q + Q - 8 : m * Q + Q, :conv_cols] for m in range(2)]
        is_last = (x_at + distance) % x_size == x_size - 1
        edge = jnp.where(is_last, jnp.where(c_at == 1, ends[0], ends[1]), edge)
        pairs.append(pair)
        firsts.append(first)
    halo = later(edge, SEQ, 1)
    xc, bc, dt, cumul, last = summarize(
        dt_bias, decay_rate, firsts, halo, conv_x, conv_bc, heads, width, bc_cols
    )
    pairs[3], w_out, last = lax.optimization_barrier((pairs[3], w_out, last))
    z_size = lax.axis_size("z")
    pieces = lax.all_to_all(
        last.reshape(z_size, Q // z_size, width + Q), "z", 0, 0, tiled=True
    )
    seconds = [jnp.dot(pair, w_in_z, preferred_element_type=F32) for pair in pairs]
    d_half = d_model // 2
    own_low, own_high = [
        (part.astype(F32) * norm_gain[:, None]).astype(BF16)
        for part in (w_out[:, :d_half], w_out[:, d_half:])
    ]
    w_low = (own_low, swap(own_low))
    w_high = (own_high, swap(own_high))
    ig, fz, sloc, growth = inside(skip, seconds, xc, bc, dt, cumul, heads)
    before, row_growth, row_total = row_scan(pieces, heads)
    near = later(row_total, "y", 1)
    middle = later(row_total, "y", 2)
    far = later(row_total, "y", 3)
    joined = join_rows(near, middle, far, before, row_growth, heads)
    entering = lax.all_to_all(joined, "z", 0, 0, tiled=True).reshape(Q, width)

    core = c_at.astype(jnp.int32)[None]
    away = finish(1 - core, bc, ig, fz, sloc, growth, entering)
    arrived = swap(away)
    kept = finish(core, bc, ig, fz, sloc, growth, entering)
    both = [block.reshape(x_size, own_rows, width) for block in (kept, arrived)]

    def partial(distance, weights, added=None):
        at = (x_at + distance) % x_size
        blocks = [lax.dynamic_index_in_dim(part, at, 0, keepdims=False) for part in both]
        result = sum(
            jnp.dot(block, weight, preferred_element_type=F32)
            for block, weight in zip(blocks, weights)
        )
        if added is not None:
            result = result + added.astype(F32)
        return result

    def sent(distance, weights, way, added=None):
        part = partial(distance, weights, added).astype(BF16)
        return named(part, way)

    far_low = sent(2, w_low, 1)
    far_high = sent(2, w_high, -1)
    right_high = sent(1, w_high, 1)
    left_low = sent(-1, w_low, -1)
    squares = sum(jnp.sum(jnp.square(part.astype(F32)), axis=2) for part in both)
    squares = lax.all_to_all(squares, "x", 0, 0, tiled=True)
    right_low = sent(1, w_low, 1, far_low)
    left_high = sent(-1, w_high, -1, far_high)
    low = partial(0, w_low)
    high = partial(0, w_high)
    return close(squares, low, high, right_low, left_low, right_high, left_high)


def close_kernel(squares, low, high, right_low, left_low, right_high, left_high, out):
    rows, half = low.shape
    total = jnp.sum(squares[...], axis=0, keepdims=True)
    scale = lax.rsqrt(jnp.broadcast_to(total, (rows, rows)).T / E + 1e-05)
    sides = ((low, right_low, left_low), (high, right_high, left_high))
    for side, (own, first, second) in enumerate(sides):
        for lo in range(0, half, rows):
            at = slice(lo, lo + rows)
            value = own[:, at] + first[:, at].astype(F32) + second[:, at].astype(F32)
            out[:, side * half + lo : side * half + lo + rows] = (value * scale).astype(BF16)


def close(squares, low, high, *parts):
    return pl.pallas_call(
        close_kernel,
        in_specs=vmem_specs(7, 0),
        out_shape=jax.ShapeDtypeStruct((low.shape[0], 2 * low.shape[1]), BF16),
        name="close",
    )(squares, low, high, *parts)


def solution(mesh):
    torus = Mesh(mesh.devices.reshape(4, 8, 4, 2), ALL)
    head = ("x", "c")
    placed = (
        P(ALL, None),
        P(None, head),
        P(None, head),
        P(),
        P(None, head),
        P(None, head),
        P(),
        P(head),
        P(head),
        P(head),
        P(head),
        P(head, None),
    )
    return jax.shard_map(
        per_device, mesh=torus, in_specs=placed, out_specs=P(ALL, None), check_vma=False
    )
```

```python
import jax
import jax.numpy as jnp
from jax import lax
from jax.experimental import pallas as pl
from jax.experimental.pallas import tpu as pltpu
from jax.sharding import Mesh
from jax.sharding import PartitionSpec as P


E = 4096
Q = 128
KERNEL = 4
SEQ = ("y", "z")
ALL = ("y", "z", "x", "c")
F32 = jnp.float32
BF16 = jnp.bfloat16
highest = lax.Precision.HIGHEST
LIMIT = pltpu.CompilerParams(vmem_limit_bytes=20 * 1024 * 1024)


def silu(v):
    half = 0.5 * v
    return half + half * jnp.tanh(half)


def shift(block, axis, distance):
    size = lax.axis_size(axis)
    return lax.ppermute(block, axis, [(i, (i + distance) % size) for i in range(size)])


def later(block, axis, distance):
    size = lax.axis_size(axis)
    return lax.ppermute(block, axis, [(i, i + distance) for i in range(size - distance)])


def fold(values, heads, chunk):
    lanes = values.shape[1]
    high = values.astype(BF16).astype(F32)
    low = values - high
    first = pltpu.roll(high, -chunk * heads % lanes, 1) if chunk else high
    second = pltpu.roll(low, (heads - chunk * heads) % lanes, 1) if chunk != 1 else low
    lane = lax.broadcasted_iota(jnp.int32, values.shape, 1)
    return jnp.where(lane < heads, first, second).astype(BF16)


def widen(values, heads, chunk, spread):
    return jnp.dot(fold(values, heads, chunk), spread, preferred_element_type=F32)


def spread_of(heads, width):
    line = lax.broadcasted_iota(jnp.int32, (Q, width), 0)
    lane = lax.broadcasted_iota(jnp.int32, (Q, width), 1)
    hit = (line % heads == lane // (width // heads)) & (line < 2 * heads)
    return jnp.where(hit, 1.0, 0.0).astype(BF16)


def lanes_of(scalars, heads, limit):
    lane = lax.broadcasted_iota(jnp.int32, (1, Q), 1)
    row = jnp.zeros((1, Q), F32)
    for head in range(heads):
        row = jnp.where(lane % heads == head, scalars[head], row)
    return jnp.where(lane < limit, row, 0.0)


def starts_of(chunks):
    size = chunks // 2
    x_at, c_at = lax.axis_index("x"), lax.axis_index("c")
    places = []
    for distance in (0, size - 1, 1, 2):
        moved = x_at + distance
        place = jnp.where(moved >= size, moved - size, moved) * 2
        places += [(place + c_at) * Q, (place + 1 - c_at) * Q]
    return places


def three_rows(whole):
    row = lax.broadcasted_iota(jnp.int32, whole.shape, 0) % 16
    high = whole.astype(BF16).astype(F32)
    middle = (whole - high).astype(BF16).astype(F32)
    low = whole - high - middle
    return jnp.where(
        row == 0, high, jnp.where(row == 1, middle, jnp.where(row == 2, low, 0.0))
    ).astype(BF16)


def summary_kernel(heads, chunks):
    def kernel(
        bias, rate, g0, g1, g2, g3, halo, taps_x, taps_bc,
        xc_out, bc_out, dt_out, cum_out, last_out, window, scaled,
    ):
        width = xc_out.shape[1]
        conv_cols = width + bc_out.shape[1]
        starts = starts_of(chunks)
        for group, ref in enumerate((g0, g1, g2, g3)):
            for member in range(2):
                at = pl.multiple_of(starts[2 * group + member] + 8, 8)
                window[pl.ds(at, Q), :] = ref[member * Q : member * Q + Q, :].astype(F32)
        window[0:8, :conv_cols] = halo[...].astype(F32)[8:16, :]
        spread = spread_of(heads, width)
        row = lax.broadcasted_iota(jnp.int32, (Q, Q), 0)
        col = lax.broadcasted_iota(jnp.int32, (Q, Q), 1)
        tri = jnp.where(row >= col, 1.0, 0.0)
        taps = jnp.concatenate([taps_x[...], taps_bc[...]], axis=1)
        lane = lax.broadcasted_iota(jnp.int32, (Q, Q), 1)
        raw = jnp.zeros((Q, Q), F32)
        for chunk in range(chunks):
            lo = 8 + chunk * Q
            part = window[lo : lo + Q, conv_cols:]
            part = pltpu.roll(part, chunk * heads, 1) if chunk else part
            raw = jnp.where(lane // heads == chunk, part, raw)
        raw = raw + lanes_of(bias, heads, chunks * heads)
        dt = jnp.maximum(raw, 0.0) + jnp.log1p(jnp.exp(-jnp.abs(raw)))
        log_decay = -dt * lanes_of(rate, heads, chunks * heads)
        cumul = jnp.dot(tri, log_decay, precision=highest, preferred_element_type=F32)
        dt_out[...] = dt
        cum_out[...] = cumul
        total = cumul[Q - 1 : Q, :]
        suffix = jnp.zeros((8, Q), F32)
        wide_total = jnp.broadcast_to(total, (8, Q))
        for k in range(1, chunks):
            suffix = suffix + pltpu.roll(wide_total, Q - k * heads, 1)
        suffix = suffix[0:1, :]
        weight = dt * jnp.exp(jnp.minimum(total - cumul + suffix, 0.0))
        for chunk in range(chunks):
            lo = 8 + chunk * Q
            conv = taps[3:4, :] * window[lo : lo + Q, :conv_cols]
            for back in range(1, KERNEL):
                conv += taps[3 - back : 4 - back, :] * window[lo - back : lo - back + Q, :conv_cols]
            act = silu(conv)
            xc_out[lo - 8 : lo - 8 + Q, :] = act[:, :width].astype(BF16)
            bc_out[lo - 8 : lo - 8 + Q, :] = act[:, width:].astype(BF16)
            wide = widen(weight, heads, chunk, spread)
            scaled[lo - 8 : lo - 8 + Q, :] = (act[:, :width] * wide).astype(BF16)
        last_out[:, :width] = lax.dot_general(
            bc_out[:, :Q], scaled[...], (((0,), (0,)), ((), ())), preferred_element_type=F32
        ).astype(BF16)
        last_out[:, width:] = three_rows(jnp.broadcast_to(total + suffix, (Q, Q)))

    return kernel


def vmem_specs(count, scalars=1):
    return [pl.BlockSpec(memory_space=pltpu.SMEM)] * scalars + [
        pl.BlockSpec(memory_space=pltpu.VMEM)
    ] * count


def summarize(bias, rate, groups, halo, taps_x, taps_bc, heads, width, bc_cols):
    rows = 8 * Q
    return pl.pallas_call(
        summary_kernel(heads, rows // Q),
        in_specs=vmem_specs(7, 2),
        out_specs=vmem_specs(5, 0),
        out_shape=[
            jax.ShapeDtypeStruct((rows, width), BF16),
            jax.ShapeDtypeStruct((rows, bc_cols), BF16),
            jax.ShapeDtypeStruct((Q, Q), F32),
            jax.ShapeDtypeStruct((Q, Q), F32),
            jax.ShapeDtypeStruct((Q, width + Q), BF16),
        ],
        scratch_shapes=[
            pltpu.VMEM((rows + 8, groups[0].shape[1]), F32),
            pltpu.VMEM((rows, width), BF16),
        ],
        cost_estimate=pl.CostEstimate(
            flops=3_000_000_000, bytes_accessed=8_000_000, transcendentals=1_000_000
        ),
        compiler_params=LIMIT,
        name="summarize",
    )(bias, rate, *groups, halo, taps_x, taps_bc)


def inside_kernel(heads, chunks, lead):
    def kernel(
        skip, g0, g1, g2, g3, xc, bc, dt_in, cum_in, state_in,
        ig_out, fz_out, sloc_out, growth_out, state_out, gate,
    ):
        width = xc.shape[1]
        pair = 2 * (width // heads)
        spread = spread_of(heads, width)
        starts = starts_of(chunks)
        for group, ref in enumerate((g0, g1, g2, g3)):
            for member in range(2):
                at = pl.multiple_of(starts[2 * group + member], Q)
                gate[pl.ds(at, Q), :] = ref[member * Q : member * Q + Q, :]
        row = lax.broadcasted_iota(jnp.int32, (Q, Q), 0)
        col = lax.broadcasted_iota(jnp.int32, (Q, Q), 1)
        lower = row >= col
        lane = lax.broadcasted_iota(jnp.int32, (Q, pair), 1)
        zero = jnp.zeros((Q, pair), BF16)
        dt = dt_in[...]
        cumul = cum_in[...]
        flipped = cumul.T
        total = cumul[Q - 1 : Q, :]
        weight = dt * jnp.exp(jnp.minimum(total - cumul, 0.0))
        reach = jnp.exp(cumul)
        wide_total = jnp.broadcast_to(total, (8, Q))
        prefix = jnp.zeros((8, Q), F32)
        for k in range(1, chunks):
            prefix = prefix + pltpu.roll(wide_total, k * heads, 1)
        grown = jnp.exp(prefix)
        decay = jnp.exp(wide_total)
        rows8 = lax.broadcasted_iota(jnp.int32, (8, Q), 0)
        grown_rows = jnp.zeros((8, Q), F32)
        decay_rows = jnp.zeros((8, Q), F32)
        for chunk in range(chunks):
            turn = -chunk * heads % Q
            grown_rows = jnp.where(
                rows8 == chunk, pltpu.roll(grown, turn, 1) if turn else grown, grown_rows
            )
            decay_rows = jnp.where(
                rows8 == chunk, pltpu.roll(decay, turn, 1) if turn else decay, decay_rows
            )
        growth_out[...] = widen(grown_rows, heads, 0, spread)
        decay_wide = widen(decay_rows, heads, 0, spread)
        state = state_in[...] if lead else jnp.zeros((Q, width), F32)
        for local in range(chunks // 2):
            chunk = lead + local
            at = slice(local * Q, local * Q + Q)
            place = slice(chunk * Q, chunk * Q + Q)
            b_rows = bc[place, :Q]
            c_rows = bc[place, Q:]
            x = xc[place, :].astype(F32)
            sloc_out[local] = state.astype(BF16)
            if chunk < chunks - 1:
                kept = (x * widen(weight, heads, chunk, spread)).astype(BF16)
                fresh = lax.dot_general(
                    b_rows, kept, (((0,), (0,)), ((), ())), preferred_element_type=F32
                )
                state = decay_wide[chunk : chunk + 1, :] * state + fresh
            scores = lax.dot_general(
                c_rows, b_rows, (((1,), (1,)), ((), ())), preferred_element_type=F32
            )
            scores = jnp.where(lower, scores, 0.0)
            scaled = (x * widen(dt, heads, chunk, spread)).astype(BF16)
            act = silu(gate[chunk * Q : chunk * Q + Q, :].astype(F32))
            fz_out[at, :] = (widen(reach, heads, chunk, spread) * act).astype(BF16)
            for first in range(0, heads, 2):
                parts = []
                for head in (first, first + 1):
                    k = chunk * heads + head
                    gap = cumul[:, k : k + 1] - flipped[k : k + 1, :]
                    parts.append((scores * jnp.exp(jnp.minimum(gap, 0.0))).astype(BF16))
                lo = (first // 2) * pair
                block = scaled[:, lo : lo + pair]
                stacked = jnp.concatenate(
                    [
                        jnp.where(lane < pair // 2, block, zero),
                        jnp.where(lane < pair // 2, zero, block),
                    ],
                    axis=0,
                )
                out = jnp.dot(
                    jnp.concatenate(parts, axis=1), stacked, preferred_element_type=F32
                )
                coefficient = jnp.where(lane < pair // 2, skip[first], skip[first + 1])
                out = out + coefficient * x[:, lo : lo + pair]
                ig_out[at, lo : lo + pair] = (out * act[:, lo : lo + pair]).astype(BF16)
        state_out[...] = state

    return kernel


def inside(skip, groups, xc, bc, dt, cumul, state, heads, part):
    rows, width = xc.shape
    chunks = rows // Q
    half = rows // 2
    return pl.pallas_call(
        inside_kernel(heads, chunks, part * chunks // 2),
        in_specs=vmem_specs(9),
        out_specs=vmem_specs(5, 0),
        out_shape=[
            jax.ShapeDtypeStruct((half, width), BF16),
            jax.ShapeDtypeStruct((half, width), BF16),
            jax.ShapeDtypeStruct((chunks // 2, Q, width), BF16),
            jax.ShapeDtypeStruct((8, width), F32),
            jax.ShapeDtypeStruct((Q, width), F32),
        ],
        scratch_shapes=[pltpu.VMEM((rows, width), BF16)],
        cost_estimate=pl.CostEstimate(
            flops=4_000_000_000, bytes_accessed=5_000_000, transcendentals=1_000_000
        ),
        compiler_params=LIMIT,
        name="inside",
    )(skip, *groups, xc, bc, dt, cumul, state)


def finish_kernel(away):
    def kernel(bc, ig0, fz0, sloc0, ig1, fz1, sloc1, growth, entering, out):
        start = entering[...].astype(F32)
        c_at = lax.axis_index("c")
        offset = 1 - c_at if away else c_at
        for i in range(4):
            ig, fz, sloc = ((ig0, fz0, sloc0), (ig1, fz1, sloc1))[i // 2]
            chunk = 2 * i + offset
            local = 2 * (i % 2) + offset
            at = pl.ds(pl.multiple_of(local * Q, Q), Q)
            state = sloc[local].astype(F32) + growth[pl.ds(chunk, 1), :] * start
            c_rows = bc[pl.ds(pl.multiple_of(chunk * Q, Q), Q), Q:]
            carried = jnp.dot(c_rows, state.astype(BF16), preferred_element_type=F32)
            out[i * Q : i * Q + Q, :] = (
                ig[at, :].astype(F32) + carried * fz[at, :].astype(F32)
            ).astype(BF16)

    return kernel


def finish(away, bc, early, late, growth, entering):
    shape = (bc.shape[0] // 2, entering.shape[1])
    return pl.pallas_call(
        finish_kernel(away),
        in_specs=vmem_specs(9, 0),
        out_specs=pl.BlockSpec(memory_space=pltpu.VMEM),
        out_shape=jax.ShapeDtypeStruct(shape, BF16),
        cost_estimate=pl.CostEstimate(
            flops=1_500_000_000, bytes_accessed=3_000_000, transcendentals=0
        ),
        compiler_params=LIMIT,
        name="finish",
    )(bc, *early, *late, growth, entering)


def project_kernel(distances):
    def kernel(kept, arrived, own_low, other_low, own_high, other_high, *refs):
        lows, highs = refs[: len(distances)], refs[len(distances) : -1]
        rows_in = refs[-1]
        width = kept.shape[1]
        size = kept.shape[0] // Q
        columns = own_low.shape[1]
        x_at = lax.axis_index("x")
        for place, distance in enumerate(distances):
            moved = x_at + distance
            block = jnp.where(moved >= size, moved - size, moved)
            at = pl.ds(pl.multiple_of(block * Q, Q), Q)
            lines = slice(place * Q, place * Q + Q)
            rows_in[lines, :width] = kept[at, :]
            rows_in[lines, width:] = arrived[at, :]
            wide = rows_in[lines, :].astype(F32)
            each = jnp.sum(wide * wide, axis=1, keepdims=True)
            lows[place][:, columns:] = jnp.broadcast_to(each, (Q, Q)).astype(BF16)
        for own, other, outs in ((own_low, other_low, lows), (own_high, other_high, highs)):
            for lo in range(0, columns, 256):
                tile = slice(lo, lo + 256)
                result = jnp.dot(rows_in[:, :width], own[:, tile], preferred_element_type=F32)
                result += jnp.dot(rows_in[:, width:], other[:, tile], preferred_element_type=F32)
                result = result.astype(BF16)
                for place, out in enumerate(outs):
                    out[:, tile] = result[place * Q : place * Q + Q, :]

    return kernel


def project(kept, arrived, weights, distances):
    width = kept.shape[1]
    columns = weights[0].shape[1]
    count = len(distances)
    vmem = pl.BlockSpec(memory_space=pltpu.VMEM)
    low = jax.ShapeDtypeStruct((Q, columns + Q), BF16)
    high = jax.ShapeDtypeStruct((Q, columns), BF16)
    return pl.pallas_call(
        project_kernel(distances),
        in_specs=[vmem] * 6,
        out_specs=[vmem] * (2 * count),
        out_shape=[low] * count + [high] * count,
        scratch_shapes=[pltpu.VMEM((count * Q, 2 * width), BF16)],
        cost_estimate=pl.CostEstimate(
            flops=1_000_000_000 * count, bytes_accessed=5_000_000, transcendentals=0
        ),
        compiler_params=LIMIT,
        name="project",
    )(kept, arrived, *weights)


def row_kernel(heads):
    def kernel(pieces, before_out, growth_out, row_out):
        width = before_out.shape[2]
        spread = spread_of(heads, width)
        count = pieces.shape[0]
        rows8 = lax.broadcasted_iota(jnp.int32, (8, Q), 0)
        parts = jnp.zeros((8, Q), F32)
        sums = jnp.zeros((8, Q), F32)
        total = jnp.zeros((1, Q), F32)
        for k in range(count):
            tail = pieces[k, :, width:].astype(F32)
            part = tail[0:1] + tail[1:2] + tail[2:3]
            parts = jnp.where(rows8 == k, part, parts)
            sums = jnp.where(rows8 == k, total, sums)
            total = total + part
        growth_out[...] = widen(jnp.exp(sums), heads, 0, spread)
        decay = widen(jnp.exp(parts), heads, 0, spread)
        state = jnp.zeros(before_out.shape[1:], F32)
        for k in range(count):
            before_out[k] = state
            state = decay[k : k + 1] * state + pieces[k, :, :width].astype(F32)
        row_out[:, :width] = state.astype(BF16)
        row_out[:, width:] = three_rows(jnp.broadcast_to(total, (16, Q)))

    return kernel


def row_scan(pieces, heads):
    count, rows, cols = pieces.shape
    width = cols - Q
    return pl.pallas_call(
        row_kernel(heads),
        in_specs=vmem_specs(1, 0),
        out_shape=[
            jax.ShapeDtypeStruct((count, rows, width), F32),
            jax.ShapeDtypeStruct((8, width), F32),
            jax.ShapeDtypeStruct((rows, cols), BF16),
        ],
        compiler_params=LIMIT,
        name="row_scan",
    )(pieces)


def join_kernel(heads):
    def kernel(near, middle, far, before, growth, out):
        width = out.shape[2]
        spread = spread_of(heads, width)

        def log_of(piece):
            tail = piece[:, width:].astype(F32)
            return tail[0:1] + tail[1:2] + tail[2:3]

        rows8 = lax.broadcasted_iota(jnp.int32, (8, Q), 0)
        logs = jnp.where(rows8 == 0, log_of(near), log_of(middle))
        decay = widen(jnp.exp(logs), heads, 0, spread)
        entering = far[:, :width].astype(F32)
        entering = decay[1:2] * entering + middle[:, :width].astype(F32)
        entering = decay[0:1] * entering + near[:, :width].astype(F32)
        for k in range(out.shape[0]):
            out[k] = (before[k] + growth[k : k + 1] * entering).astype(BF16)

    return kernel


def join_rows(near, middle, far, before, growth, heads):
    count, rows, width = before.shape
    return pl.pallas_call(
        join_kernel(heads),
        in_specs=vmem_specs(5, 0),
        out_shape=jax.ShapeDtypeStruct((count, rows, width), BF16),
        compiler_params=LIMIT,
        name="join_rows",
    )(near, middle, far, before, growth)


def per_device(
    tokens, w_in_x, w_in_z, w_in_bc, w_dt, conv_x, conv_bc,
    dt_bias, decay_rate, skip, norm_gain, w_out,
):
    width = w_in_x.shape[1]
    heads = dt_bias.shape[0]
    bc_cols = w_in_bc.shape[1]
    own_rows, d_model = tokens.shape
    half = own_rows // 2
    x_size = lax.axis_size("x")
    x_at = lax.axis_index("x")
    c_at = lax.axis_index("c")
    swap = lambda block: shift(block, "c", 1)

    top, bottom = tokens[:half], tokens[half:]

    def named(block, distance, axis="x"):
        return shift(block, axis, distance)

    left_top = named(top, 1)
    right_bottom = named(bottom, -1)
    left_bottom = named(bottom, 1)
    right_top = named(top, -1)
    far_top = named(left_top, 1)
    far_bottom = named(right_bottom, -1)

    w_first = jnp.concatenate(
        [w_in_x, w_in_bc, w_dt, jnp.zeros((d_model, Q - heads), BF16)], axis=1
    )
    groups = (
        (0, (tokens, swap(tokens))),
        (
            -1,
            (left_top, left_bottom, named(left_top, 1, "c"), named(left_bottom, 1, "c")),
        ),
        (
            1,
            (right_top, right_bottom, named(right_top, 1, "c"), named(right_bottom, 1, "c")),
        ),
        (
            2,
            (far_top, far_bottom, named(far_top, 1, "c"), named(far_bottom, 1, "c")),
        ),
    )
    conv_cols = width + bc_cols
    pairs, firsts = [], []
    edge = jnp.zeros((16, conv_cols), BF16)
    for distance, blocks in groups:
        pair = jnp.concatenate(blocks, axis=0)
        first = jnp.dot(pair, w_first, preferred_element_type=F32).astype(BF16)
        ends = [first[m * Q + Q - 16 : m * Q + Q, :conv_cols] for m in range(2)]
        is_last = (x_at + distance) % x_size == x_size - 1
        edge = jnp.where(is_last, jnp.where(c_at == 1, ends[0], ends[1]), edge)
        pairs.append(pair)
        firsts.append(first)
    halo = later(edge, SEQ, 1)
    xc, bc, dt, cumul, last = summarize(
        dt_bias, decay_rate, firsts, halo, conv_x, conv_bc, heads, width, bc_cols
    )
    pairs[3], last = lax.optimization_barrier((pairs[3], last))
    z_size = lax.axis_size("z")
    pieces = lax.all_to_all(
        last.reshape(z_size, Q // z_size, width + Q), "z", 0, 0, tiled=True
    )
    seconds = []
    for pair in pairs:
        second = jnp.dot(pair, w_in_z, preferred_element_type=F32)
        seconds.append(second.astype(BF16))
    d_half = d_model // 2
    gained = [
        (part.astype(F32) * norm_gain[:, None]).astype(BF16)
        for part in (w_out[:, :d_half], w_out[:, d_half:])
    ]
    weights = [(part, swap(part)) for part in gained]
    *early, _, halfway = inside(skip, seconds, xc, bc, dt, cumul, dt, heads, 0)
    pieces, early = lax.optimization_barrier((pieces, early))
    *late, growth, _ = inside(skip, seconds, xc, bc, dt, cumul, halfway, heads, 1)
    before, row_growth, row_total = row_scan(pieces, heads)
    near = later(row_total, "y", 1)
    middle = later(row_total, "y", 2)
    far = later(row_total, "y", 3)
    joined = join_rows(near, middle, far, before, row_growth, heads)
    entering = lax.all_to_all(joined, "z", 0, 0, tiled=True).reshape(Q, width)

    away = finish(True, bc, early, late, growth, entering)
    arrived = swap(away)
    kept = finish(False, bc, early, late, growth, entering)
    weights = [*weights[0], *weights[1]]
    far_low, far_high = project(kept, arrived, weights, (2,))
    right_low, left_low, low, right_high, left_high, high = project(
        kept, arrived, weights, (1, x_size - 1, 0)
    )
    far_low = named(far_low, 1)
    far_high = named(far_high, -1)
    right_high = named(right_high, 1)
    left_low = named(left_low, -1)
    right_low = (right_low.astype(F32) + far_low.astype(F32)).astype(BF16)
    right_low = named(right_low, 1)
    left_high = (left_high.astype(F32) + far_high.astype(F32)).astype(BF16)
    left_high = named(left_high, -1)
    return close(low, high, right_low, left_low, right_high, left_high)


def close_kernel(low, high, right_low, left_low, right_high, left_high, out):
    _, half = high.shape
    past = slice(half, half + Q)
    total = low[:, past].astype(F32) + right_low[:, past].astype(F32)
    total += left_low[:, past].astype(F32)
    scale = lax.rsqrt(total / E + 1e-05)
    sides = ((low, right_low, left_low), (high, right_high, left_high))
    for side, (own, first, second) in enumerate(sides):
        for lo in range(0, half, Q):
            at = slice(lo, lo + Q)
            value = own[:, at].astype(F32) + first[:, at].astype(F32) + second[:, at].astype(F32)
            out[:, side * half + lo : side * half + lo + Q] = (value * scale).astype(BF16)


def close(low, high, *parts):
    return pl.pallas_call(
        close_kernel,
        in_specs=vmem_specs(6, 0),
        out_shape=jax.ShapeDtypeStruct((high.shape[0], 2 * high.shape[1]), BF16),
        compiler_params=LIMIT,
        name="close",
    )(low, high, *parts)


def solution(mesh):
    torus = Mesh(mesh.devices.reshape(4, 8, 4, 2), ALL)
    head = ("x", "c")
    placed = (
        P(ALL, None),
        P(None, head),
        P(None, head),
        P(),
        P(None, head),
        P(None, head),
        P(),
        P(head),
        P(head),
        P(head),
        P(head),
        P(head, None),
    )
    return jax.shard_map(
        per_device, mesh=torus, in_specs=placed, out_specs=P(ALL, None), check_vma=False
    )
```

```python
import jax
import jax.numpy as jnp
from jax import lax
from jax.experimental import pallas as pl
from jax.experimental.pallas import tpu as pltpu
from jax.sharding import Mesh
from jax.sharding import PartitionSpec as P


E = 4096
Q = 128
KERNEL = 4
SEQ = ("y", "z")
ALL = ("y", "z", "x", "c")
F32 = jnp.float32
BF16 = jnp.bfloat16
highest = lax.Precision.HIGHEST
LIMIT = pltpu.CompilerParams(vmem_limit_bytes=20 * 1024 * 1024)


def silu(v):
    half = 0.5 * v
    return half + half * jnp.tanh(half)


def shift(block, axis, distance):
    size = lax.axis_size(axis)
    return lax.ppermute(block, axis, [(i, (i + distance) % size) for i in range(size)])


def later(block, axis, distance):
    size = lax.axis_size(axis)
    return lax.ppermute(block, axis, [(i, i + distance) for i in range(size - distance)])


def fold(values, heads, chunk):
    lanes = values.shape[1]
    high = values.astype(BF16).astype(F32)
    low = values - high
    first = pltpu.roll(high, -chunk * heads % lanes, 1) if chunk else high
    second = pltpu.roll(low, (heads - chunk * heads) % lanes, 1) if chunk != 1 else low
    lane = lax.broadcasted_iota(jnp.int32, values.shape, 1)
    return jnp.where(lane < heads, first, second).astype(BF16)


def widen(values, heads, chunk, spread):
    return jnp.dot(fold(values, heads, chunk), spread, preferred_element_type=F32)


def spread_of(heads, width):
    line = lax.broadcasted_iota(jnp.int32, (Q, width), 0)
    lane = lax.broadcasted_iota(jnp.int32, (Q, width), 1)
    hit = (line % heads == lane // (width // heads)) & (line < 2 * heads)
    return jnp.where(hit, 1.0, 0.0).astype(BF16)


def lanes_of(scalars, heads, limit):
    lane = lax.broadcasted_iota(jnp.int32, (1, Q), 1)
    row = jnp.zeros((1, Q), F32)
    for head in range(heads):
        row = jnp.where(lane % heads == head, scalars[head], row)
    return jnp.where(lane < limit, row, 0.0)


def starts_of(chunks):
    size = chunks // 2
    x_at, c_at = lax.axis_index("x"), lax.axis_index("c")
    places = []
    for distance in (0, size - 1, 1, 2):
        moved = x_at + distance
        place = jnp.where(moved >= size, moved - size, moved) * 2
        places += [(place + c_at) * Q, (place + 1 - c_at) * Q]
    return places


def three_rows(whole):
    row = lax.broadcasted_iota(jnp.int32, whole.shape, 0) % 16
    high = whole.astype(BF16).astype(F32)
    middle = (whole - high).astype(BF16).astype(F32)
    low = whole - high - middle
    return jnp.where(
        row == 0, high, jnp.where(row == 1, middle, jnp.where(row == 2, low, 0.0))
    ).astype(BF16)


def summary_kernel(heads, chunks):
    def kernel(
        bias, rate, g0, g1, g2, g3, halo, taps_x, taps_bc,
        xc_out, bc_out, dt_out, cum_out, last_out, window, scaled,
    ):
        width = xc_out.shape[1]
        conv_cols = width + bc_out.shape[1]
        starts = starts_of(chunks)
        for group, ref in enumerate((g0, g1, g2, g3)):
            for member in range(2):
                at = pl.multiple_of(starts[2 * group + member] + 8, 8)
                window[pl.ds(at, Q), :] = ref[member * Q : member * Q + Q, :].astype(F32)
        window[0:8, :conv_cols] = halo[...].astype(F32)[8:16, :]
        spread = spread_of(heads, width)
        row = lax.broadcasted_iota(jnp.int32, (Q, Q), 0)
        col = lax.broadcasted_iota(jnp.int32, (Q, Q), 1)
        tri = jnp.where(row >= col, 1.0, 0.0)
        taps = jnp.concatenate([taps_x[...], taps_bc[...]], axis=1)
        lane = lax.broadcasted_iota(jnp.int32, (Q, Q), 1)
        raw = jnp.zeros((Q, Q), F32)
        for chunk in range(chunks):
            lo = 8 + chunk * Q
            part = window[lo : lo + Q, conv_cols:]
            part = pltpu.roll(part, chunk * heads, 1) if chunk else part
            raw = jnp.where(lane // heads == chunk, part, raw)
        raw = raw + lanes_of(bias, heads, chunks * heads)
        dt = jnp.maximum(raw, 0.0) + jnp.log1p(jnp.exp(-jnp.abs(raw)))
        log_decay = -dt * lanes_of(rate, heads, chunks * heads)
        cumul = jnp.dot(tri, log_decay, precision=highest, preferred_element_type=F32)
        dt_out[...] = dt
        cum_out[...] = cumul
        total = cumul[Q - 1 : Q, :]
        suffix = jnp.zeros((8, Q), F32)
        wide_total = jnp.broadcast_to(total, (8, Q))
        for k in range(1, chunks):
            suffix = suffix + pltpu.roll(wide_total, Q - k * heads, 1)
        suffix = suffix[0:1, :]
        weight = dt * jnp.exp(jnp.minimum(total - cumul + suffix, 0.0))
        for chunk in range(chunks):
            lo = 8 + chunk * Q
            conv = taps[3:4, :] * window[lo : lo + Q, :conv_cols]
            for back in range(1, KERNEL):
                conv += taps[3 - back : 4 - back, :] * window[lo - back : lo - back + Q, :conv_cols]
            act = silu(conv)
            xc_out[lo - 8 : lo - 8 + Q, :] = act[:, :width].astype(BF16)
            bc_out[lo - 8 : lo - 8 + Q, :] = act[:, width:].astype(BF16)
            wide = widen(weight, heads, chunk, spread)
            scaled[lo - 8 : lo - 8 + Q, :] = (act[:, :width] * wide).astype(BF16)
        last_out[:, :width] = lax.dot_general(
            bc_out[:, :Q], scaled[...], (((0,), (0,)), ((), ())), preferred_element_type=F32
        ).astype(BF16)
        last_out[:, width:] = three_rows(jnp.broadcast_to(total + suffix, (Q, Q)))

    return kernel


def vmem_specs(count, scalars=1):
    return [pl.BlockSpec(memory_space=pltpu.SMEM)] * scalars + [
        pl.BlockSpec(memory_space=pltpu.VMEM)
    ] * count


def summarize(bias, rate, groups, halo, taps_x, taps_bc, heads, width, bc_cols):
    rows = 8 * Q
    return pl.pallas_call(
        summary_kernel(heads, rows // Q),
        in_specs=vmem_specs(7, 2),
        out_specs=vmem_specs(5, 0),
        out_shape=[
            jax.ShapeDtypeStruct((rows, width), BF16),
            jax.ShapeDtypeStruct((rows, bc_cols), BF16),
            jax.ShapeDtypeStruct((Q, Q), F32),
            jax.ShapeDtypeStruct((Q, Q), F32),
            jax.ShapeDtypeStruct((Q, width + Q), BF16),
        ],
        scratch_shapes=[
            pltpu.VMEM((rows + 8, groups[0].shape[1]), F32),
            pltpu.VMEM((rows, width), BF16),
        ],
        cost_estimate=pl.CostEstimate(
            flops=3_000_000_000, bytes_accessed=8_000_000, transcendentals=1_000_000
        ),
        name="summarize",
    )(bias, rate, *groups, halo, taps_x, taps_bc)


def inside_kernel(heads, chunks, lead):
    def kernel(
        skip, g0, g1, g2, g3, xc, bc, dt_in, cum_in, state_in,
        ig_out, fz_out, sloc_out, growth_out, state_out, gate,
    ):
        width = xc.shape[1]
        pair = 2 * (width // heads)
        spread = spread_of(heads, width)
        starts = starts_of(chunks)
        for group, ref in enumerate((g0, g1, g2, g3)):
            for member in range(2):
                at = pl.multiple_of(starts[2 * group + member], Q)
                gate[pl.ds(at, Q), :] = ref[member * Q : member * Q + Q, :]
        row = lax.broadcasted_iota(jnp.int32, (Q, Q), 0)
        col = lax.broadcasted_iota(jnp.int32, (Q, Q), 1)
        lower = row >= col
        lane = lax.broadcasted_iota(jnp.int32, (Q, pair), 1)
        zero = jnp.zeros((Q, pair), BF16)
        dt = dt_in[...]
        cumul = cum_in[...]
        flipped = cumul.T
        total = cumul[Q - 1 : Q, :]
        weight = dt * jnp.exp(jnp.minimum(total - cumul, 0.0))
        reach = jnp.exp(cumul)
        wide_total = jnp.broadcast_to(total, (8, Q))
        prefix = jnp.zeros((8, Q), F32)
        for k in range(1, chunks):
            prefix = prefix + pltpu.roll(wide_total, k * heads, 1)
        grown = jnp.exp(prefix)
        decay = jnp.exp(wide_total)
        rows8 = lax.broadcasted_iota(jnp.int32, (8, Q), 0)
        grown_rows = jnp.zeros((8, Q), F32)
        decay_rows = jnp.zeros((8, Q), F32)
        for chunk in range(chunks):
            turn = -chunk * heads % Q
            grown_rows = jnp.where(
                rows8 == chunk, pltpu.roll(grown, turn, 1) if turn else grown, grown_rows
            )
            decay_rows = jnp.where(
                rows8 == chunk, pltpu.roll(decay, turn, 1) if turn else decay, decay_rows
            )
        growth_out[...] = widen(grown_rows, heads, 0, spread)
        decay_wide = widen(decay_rows, heads, 0, spread)
        state = state_in[...] if lead else jnp.zeros((Q, width), F32)
        for local in range(chunks // 2):
            chunk = lead + local
            at = slice(local * Q, local * Q + Q)
            b_rows = bc[at, :Q]
            c_rows = bc[at, Q:]
            x = xc[at, :].astype(F32)
            sloc_out[local] = state.astype(BF16)
            if chunk < chunks - 1:
                kept = (x * widen(weight, heads, chunk, spread)).astype(BF16)
                fresh = lax.dot_general(
                    b_rows, kept, (((0,), (0,)), ((), ())), preferred_element_type=F32
                )
                state = decay_wide[chunk : chunk + 1, :] * state + fresh
            scores = lax.dot_general(
                c_rows, b_rows, (((1,), (1,)), ((), ())), preferred_element_type=F32
            )
            scores = jnp.where(lower, scores, 0.0)
            scaled = (x * widen(dt, heads, chunk, spread)).astype(BF16)
            act = silu(gate[chunk * Q : chunk * Q + Q, :].astype(F32))
            fz_out[at, :] = (widen(reach, heads, chunk, spread) * act).astype(BF16)
            for first in range(0, heads, 2):
                parts = []
                for head in (first, first + 1):
                    k = chunk * heads + head
                    gap = cumul[:, k : k + 1] - flipped[k : k + 1, :]
                    parts.append((scores * jnp.exp(jnp.minimum(gap, 0.0))).astype(BF16))
                lo = (first // 2) * pair
                block = scaled[:, lo : lo + pair]
                stacked = jnp.concatenate(
                    [
                        jnp.where(lane < pair // 2, block, zero),
                        jnp.where(lane < pair // 2, zero, block),
                    ],
                    axis=0,
                )
                out = jnp.dot(
                    jnp.concatenate(parts, axis=1), stacked, preferred_element_type=F32
                )
                coefficient = jnp.where(lane < pair // 2, skip[first], skip[first + 1])
                out = out + coefficient * x[:, lo : lo + pair]
                ig_out[at, lo : lo + pair] = (out * act[:, lo : lo + pair]).astype(BF16)
        state_out[...] = state

    return kernel


def inside(skip, groups, xc, bc, dt, cumul, state, heads, part):
    rows, width = xc.shape
    chunks = rows // Q
    half = rows // 2
    whole = lambda array: pl.BlockSpec(array.shape, lambda i: (0, 0))
    near = lambda array: pl.BlockSpec((half, array.shape[1]), lambda i: (part, 0))
    shapes = [
        jax.ShapeDtypeStruct((half, width), BF16),
        jax.ShapeDtypeStruct((half, width), BF16),
        jax.ShapeDtypeStruct((chunks // 2, Q, width), BF16),
        jax.ShapeDtypeStruct((8, width), F32),
        jax.ShapeDtypeStruct((Q, width), F32),
    ]
    return pl.pallas_call(
        inside_kernel(heads, chunks, part * chunks // 2),
        grid=(1,),
        in_specs=[pl.BlockSpec(memory_space=pltpu.SMEM)]
        + [whole(group) for group in groups]
        + [near(xc), near(bc), whole(dt), whole(cumul), whole(state)],
        out_specs=[
            pl.BlockSpec(shape.shape, lambda i, n=len(shape.shape): (0,) * n) for shape in shapes
        ],
        out_shape=shapes,
        scratch_shapes=[pltpu.VMEM((rows, width), BF16)],
        cost_estimate=pl.CostEstimate(
            flops=4_000_000_000, bytes_accessed=5_000_000, transcendentals=1_000_000
        ),
        name="inside",
    )(skip, *groups, xc, bc, dt, cumul, state)


def finish_kernel(sel, c_rows, ig0, fz0, sloc0, ig1, fz1, sloc1, growth, entering, out):
    start = entering[...].astype(F32)
    for i in range(4):
        ig, fz, sloc = ((ig0, fz0, sloc0), (ig1, fz1, sloc1))[i // 2]
        state = sloc[i % 2, 0].astype(F32) + growth[pl.ds(2 * i + sel[0], 1), :] * start
        carried = jnp.dot(c_rows[i, 0], state.astype(BF16), preferred_element_type=F32)
        out[i * Q : i * Q + Q, :] = (
            ig[i % 2, 0].astype(F32) + carried * fz[i % 2, 0].astype(F32)
        ).astype(BF16)


def finish(sel, bc, early, late, growth, entering):
    rows, width = bc.shape[0], entering.shape[1]
    paired = lambda block: block.reshape(-1, 2, Q, block.shape[-1])
    block = pl.BlockSpec((2, 1, Q, width), lambda i, sel: (0, sel[0], 0, 0))
    return pl.pallas_call(
        finish_kernel,
        grid_spec=pltpu.PrefetchScalarGridSpec(
            num_scalar_prefetch=1,
            grid=(1,),
            in_specs=[pl.BlockSpec((4, 1, Q, Q), lambda i, sel: (0, sel[0], 0, 1))]
            + [block] * 6
            + [
                pl.BlockSpec(growth.shape, lambda i, sel: (0, 0)),
                pl.BlockSpec(entering.shape, lambda i, sel: (0, 0)),
            ],
            out_specs=pl.BlockSpec((rows // 2, width), lambda i, sel: (0, 0)),
        ),
        out_shape=jax.ShapeDtypeStruct((rows // 2, width), BF16),
        cost_estimate=pl.CostEstimate(
            flops=1_500_000_000, bytes_accessed=3_000_000, transcendentals=0
        ),
        name="finish",
    )(sel, paired(bc), *map(paired, early), *map(paired, late), growth, entering)


def project_kernel(distances):
    def kernel(kept, arrived, own_low, other_low, own_high, other_high, *refs):
        lows, highs = refs[: len(distances)], refs[len(distances) : -1]
        rows_in = refs[-1]
        width = kept.shape[1]
        size = kept.shape[0] // Q
        columns = own_low.shape[1]
        x_at = lax.axis_index("x")
        for place, distance in enumerate(distances):
            moved = x_at + distance
            block = jnp.where(moved >= size, moved - size, moved)
            at = pl.ds(pl.multiple_of(block * Q, Q), Q)
            lines = slice(place * Q, place * Q + Q)
            rows_in[lines, :width] = kept[at, :]
            rows_in[lines, width:] = arrived[at, :]
            wide = rows_in[lines, :].astype(F32)
            each = jnp.sum(wide * wide, axis=1, keepdims=True)
            lows[place][:, columns:] = jnp.broadcast_to(each, (Q, Q)).astype(BF16)
        for own, other, outs in ((own_low, other_low, lows), (own_high, other_high, highs)):
            for lo in range(0, columns, 256):
                tile = slice(lo, lo + 256)
                result = jnp.dot(rows_in[:, :width], own[:, tile], preferred_element_type=F32)
                result += jnp.dot(rows_in[:, width:], other[:, tile], preferred_element_type=F32)
                result = result.astype(BF16)
                for place, out in enumerate(outs):
                    out[:, tile] = result[place * Q : place * Q + Q, :]

    return kernel


def project(kept, arrived, weights, distances):
    width = kept.shape[1]
    columns = weights[0].shape[1]
    count = len(distances)
    vmem = pl.BlockSpec(memory_space=pltpu.VMEM)
    low = jax.ShapeDtypeStruct((Q, columns + Q), BF16)
    high = jax.ShapeDtypeStruct((Q, columns), BF16)
    return pl.pallas_call(
        project_kernel(distances),
        in_specs=[vmem] * 6,
        out_specs=[vmem] * (2 * count),
        out_shape=[low] * count + [high] * count,
        scratch_shapes=[pltpu.VMEM((count * Q, 2 * width), BF16)],
        cost_estimate=pl.CostEstimate(
            flops=1_000_000_000 * count, bytes_accessed=5_000_000, transcendentals=0
        ),
        compiler_params=LIMIT,
        name="project",
    )(kept, arrived, *weights)


def row_kernel(heads):
    def kernel(pieces, before_out, growth_out, row_out):
        width = before_out.shape[2]
        spread = spread_of(heads, width)
        count = pieces.shape[0]
        rows8 = lax.broadcasted_iota(jnp.int32, (8, Q), 0)
        parts = jnp.zeros((8, Q), F32)
        sums = jnp.zeros((8, Q), F32)
        total = jnp.zeros((1, Q), F32)
        for k in range(count):
            tail = pieces[k, :, width:].astype(F32)
            part = tail[0:1] + tail[1:2] + tail[2:3]
            parts = jnp.where(rows8 == k, part, parts)
            sums = jnp.where(rows8 == k, total, sums)
            total = total + part
        growth_out[...] = widen(jnp.exp(sums), heads, 0, spread)
        decay = widen(jnp.exp(parts), heads, 0, spread)
        state = jnp.zeros(before_out.shape[1:], F32)
        for k in range(count):
            before_out[k] = state
            state = decay[k : k + 1] * state + pieces[k, :, :width].astype(F32)
        row_out[:, :width] = state.astype(BF16)
        row_out[:, width:] = three_rows(jnp.broadcast_to(total, (16, Q)))

    return kernel


def row_scan(pieces, heads):
    count, rows, cols = pieces.shape
    width = cols - Q
    return pl.pallas_call(
        row_kernel(heads),
        in_specs=vmem_specs(1, 0),
        out_shape=[
            jax.ShapeDtypeStruct((count, rows, width), F32),
            jax.ShapeDtypeStruct((8, width), F32),
            jax.ShapeDtypeStruct((rows, cols), BF16),
        ],
        compiler_params=LIMIT,
        name="row_scan",
    )(pieces)


def join_kernel(heads):
    def kernel(near, middle, far, before, growth, out):
        width = out.shape[2]
        spread = spread_of(heads, width)

        def log_of(piece):
            tail = piece[:, width:].astype(F32)
            return tail[0:1] + tail[1:2] + tail[2:3]

        rows8 = lax.broadcasted_iota(jnp.int32, (8, Q), 0)
        logs = jnp.where(rows8 == 0, log_of(near), log_of(middle))
        decay = widen(jnp.exp(logs), heads, 0, spread)
        entering = far[:, :width].astype(F32)
        entering = decay[1:2] * entering + middle[:, :width].astype(F32)
        entering = decay[0:1] * entering + near[:, :width].astype(F32)
        for k in range(out.shape[0]):
            out[k] = (before[k] + growth[k : k + 1] * entering).astype(BF16)

    return kernel


def join_rows(near, middle, far, before, growth, heads):
    count, rows, width = before.shape
    return pl.pallas_call(
        join_kernel(heads),
        in_specs=vmem_specs(5, 0),
        out_shape=jax.ShapeDtypeStruct((count, rows, width), BF16),
        compiler_params=LIMIT,
        name="join_rows",
    )(near, middle, far, before, growth)


def per_device(
    tokens, w_in_x, w_in_z, w_in_bc, w_dt, conv_x, conv_bc,
    dt_bias, decay_rate, skip, norm_gain, w_out,
):
    width = w_in_x.shape[1]
    heads = dt_bias.shape[0]
    bc_cols = w_in_bc.shape[1]
    own_rows, d_model = tokens.shape
    half = own_rows // 2
    x_size = lax.axis_size("x")
    x_at = lax.axis_index("x")
    c_at = lax.axis_index("c")
    swap = lambda block: shift(block, "c", 1)

    top, bottom = tokens[:half], tokens[half:]

    def named(block, distance, axis="x"):
        return shift(block, axis, distance)

    left_top = named(top, 1)
    right_bottom = named(bottom, -1)
    left_bottom = named(bottom, 1)
    right_top = named(top, -1)
    far_top = named(left_top, 1)
    far_bottom = named(right_bottom, -1)

    w_first = jnp.concatenate(
        [w_in_x, w_in_bc, w_dt, jnp.zeros((d_model, Q - heads), BF16)], axis=1
    )
    groups = (
        (0, (tokens, swap(tokens))),
        (
            -1,
            (left_top, left_bottom, named(left_top, 1, "c"), named(left_bottom, 1, "c")),
        ),
        (
            1,
            (right_top, right_bottom, named(right_top, 1, "c"), named(right_bottom, 1, "c")),
        ),
        (
            2,
            (far_top, far_bottom, named(far_top, 1, "c"), named(far_bottom, 1, "c")),
        ),
    )
    conv_cols = width + bc_cols
    pairs, firsts = [], []
    edge = jnp.zeros((16, conv_cols), BF16)
    for distance, blocks in groups:
        pair = jnp.concatenate(blocks, axis=0)
        first = jnp.dot(pair, w_first, preferred_element_type=F32).astype(BF16)
        ends = [first[m * Q + Q - 16 : m * Q + Q, :conv_cols] for m in range(2)]
        is_last = (x_at + distance) % x_size == x_size - 1
        edge = jnp.where(is_last, jnp.where(c_at == 1, ends[0], ends[1]), edge)
        pairs.append(pair)
        firsts.append(first)
    halo = later(edge, SEQ, 1)
    xc, bc, dt, cumul, last = summarize(
        dt_bias, decay_rate, firsts, halo, conv_x, conv_bc, heads, width, bc_cols
    )
    pairs[3], last = lax.optimization_barrier((pairs[3], last))
    z_size = lax.axis_size("z")
    pieces = lax.all_to_all(
        last.reshape(z_size, Q // z_size, width + Q), "z", 0, 0, tiled=True
    )
    seconds = []
    for pair in pairs:
        second = jnp.dot(pair, w_in_z, preferred_element_type=F32)
        seconds.append(second.astype(BF16))
    d_half = d_model // 2
    gained = [
        (part.astype(F32) * norm_gain[:, None]).astype(BF16)
        for part in (w_out[:, :d_half], w_out[:, d_half:])
    ]
    weights = [(part, swap(part)) for part in gained]
    *early, _, halfway = inside(skip, seconds, xc, bc, dt, cumul, dt, heads, 0)
    pieces, early = lax.optimization_barrier((pieces, early))
    *late, growth, _ = inside(skip, seconds, xc, bc, dt, cumul, halfway, heads, 1)
    before, row_growth, row_total = row_scan(pieces, heads)
    near = later(row_total, "y", 1)
    middle = later(row_total, "y", 2)
    far = later(row_total, "y", 3)
    joined = join_rows(near, middle, far, before, row_growth, heads)
    entering = lax.all_to_all(joined, "z", 0, 0, tiled=True).reshape(Q, width)

    core = c_at.astype(jnp.int32)[None]
    away = finish(1 - core, bc, early, late, growth, entering)
    arrived = swap(away)
    kept = finish(core, bc, early, late, growth, entering)
    weights = [*weights[0], *weights[1]]
    far_low, far_high = project(kept, arrived, weights, (2,))
    right_low, left_low, low, right_high, left_high, high = project(
        kept, arrived, weights, (1, x_size - 1, 0)
    )
    far_low = named(far_low, 1)
    far_high = named(far_high, -1)
    right_high = named(right_high, 1)
    left_low = named(left_low, -1)
    right_low = (right_low.astype(F32) + far_low.astype(F32)).astype(BF16)
    right_low = named(right_low, 1)
    left_high = (left_high.astype(F32) + far_high.astype(F32)).astype(BF16)
    left_high = named(left_high, -1)
    return close(low, high, right_low, left_low, right_high, left_high)


def close_kernel(low, high, right_low, left_low, right_high, left_high, out):
    _, half = high.shape
    past = slice(half, half + Q)
    total = low[:, past].astype(F32) + right_low[:, past].astype(F32)
    total += left_low[:, past].astype(F32)
    scale = lax.rsqrt(total / E + 1e-05)
    sides = ((low, right_low, left_low), (high, right_high, left_high))
    for side, (own, first, second) in enumerate(sides):
        for lo in range(0, half, Q):
            at = slice(lo, lo + Q)
            value = own[:, at].astype(F32) + first[:, at].astype(F32) + second[:, at].astype(F32)
            out[:, side * half + lo : side * half + lo + Q] = (value * scale).astype(BF16)


def close(low, high, *parts):
    return pl.pallas_call(
        close_kernel,
        in_specs=vmem_specs(6, 0),
        out_shape=jax.ShapeDtypeStruct((high.shape[0], 2 * high.shape[1]), BF16),
        compiler_params=LIMIT,
        name="close",
    )(low, high, *parts)


def solution(mesh):
    torus = Mesh(mesh.devices.reshape(4, 8, 4, 2), ALL)
    head = ("x", "c")
    placed = (
        P(ALL, None),
        P(None, head),
        P(None, head),
        P(),
        P(None, head),
        P(None, head),
        P(),
        P(head),
        P(head),
        P(head),
        P(head),
        P(head, None),
    )
    return jax.shard_map(
        per_device, mesh=torus, in_specs=placed, out_specs=P(ALL, None), check_vma=False
    )
```
